32 devices in a mesh: tensor: 4 (over y, core), expert: 4 (over z), dp: 2 (over x).
Axes of the slice: x: 2, y: 2, z: 4, core: 2. Of those that a mesh axis runs over, the one named last changes fastest.
Arguments:
- grad_out: bfloat16 [512, 4096], P(('expert', 'dp')), may hold values from -6 to 6
- route_ids: int32 [512, 8], P(('expert', 'dp')), may hold values from 0 to 127, all different within a row; in each aligned block of 64 rows (0 to 63, 64 to 127, ...) at most 6 rows name the same one
- route_probs: bfloat16 [512, 8], P(('expert', 'dp')), may hold values from 0.019897461 to 0.5
- gate_act: bfloat16 [2, 128, 24, 768], P('dp', 'expert', None, 'tensor'), may hold values from -8 to 8
- up_act: bfloat16 [2, 128, 24, 768], P('dp', 'expert', None, 'tensor'), may hold values from -6 to 6
- w_down: bfloat16 [128, 768, 4096], P('expert', 'tensor'), may hold values from -0.21875 to 0.21875
Outputs:
- grad_gate: bfloat16 [2, 128, 24, 768], P('dp', 'expert', None, 'tensor')
- grad_up: bfloat16 [2, 128, 24, 768], P('dp', 'expert', None, 'tensor')
- grad_w_down: bfloat16 [128, 768, 4096], P('expert', 'tensor', 'dp')
- grad_probs: float32 [512, 8], P(('expert', 'dp'))
The draws below stay inside these ranges and needn't reach their ends.
Inputs may be any that keep to these rules, and one draw needn't show every extreme that they name: `route_ids`: each row names 8 different experts. Within the 64 rows of one index pair of expert and dp no expert is named more than 6 times, and in every draw some expert is named exactly 6 times there.
All inputs are finite; a program needn't handle non-finite values.
Results may differ from the reference program's by a relative error of at most 0.009.
Values may be sent and summed in bfloat16 or wider, within the bound.
A program may use at most 192 MiB of HBM per device.

```python
import math
import jax
import jax.numpy as jnp
import numpy as np
from jax import lax

D = 4096
FF = 768
EXPERTS = 128
TOP = 8
TOK_DEV = 64
CAP = 6
SLOTS = 24
TOKENS = 512
N_EXPERT = 4
N_DP = 2


def shard_levels(own_key, extent, split, smallest, top_value):
    def one(axis_at, shards_of):
        heights = jax.random.uniform(jax.random.fold_in(jax.random.fold_in(own_key, 6), axis_at), (shards_of,), jnp.float32, smallest / len(split), top_value / len(split))
        return jnp.repeat(jnp.exp(heights), extent[axis_at] // shards_of).reshape((-1,) + (1,) * (len(extent) - axis_at - 1))

    level = one(*split[0])
    for cut in split[1:]:
        level = level * one(*cut)
    return level


def assign_block(rng, own, number, rows, count, top, most, skew):
    order = jax.random.permutation(rng, count)
    packed, ordinary = shares(count, rows * top, most, skew, True), shares(count, rows * top, most, skew, False)
    places = jnp.arange(count)

    def named(lengths, offset_by):
        used = int((lengths > 0).sum())
        fixed = max(1, used // 4)
        passed = fixed + (places - fixed + offset_by * (used - fixed)) % max(1, count - fixed)
        return jnp.zeros((count,), jnp.int32).at[order[jnp.where(places < fixed, places, passed)]].set(jnp.asarray(lengths, jnp.int32))

    lengths = jnp.where(number % 4 == 0, named(packed, number // 4), named(ordinary, number - number // 4 - 1))
    mixed = jax.random.permutation(jax.random.fold_in(own, 3), count)
    donor, receiver = mixed[0:count // 2 * 2:2], mixed[1:count // 2 * 2:2]
    room = jnp.minimum(lengths[donor] - 1, most - lengths[receiver]) // 2
    room = jnp.where((donor == order[0]) | (receiver == order[0]) | (lengths[receiver] == 0), 0, jnp.maximum(room, 0))
    passed = jax.random.randint(jax.random.fold_in(own, 4), (count // 2,), 0, 1 << 20) % (room + 1)
    lengths = lengths.at[donor].add(-passed).at[receiver].add(passed)
    labels = jnp.searchsorted(jnp.cumsum(lengths), jnp.arange(rows * top), side="right").astype(jnp.int32)
    grid = labels.reshape(top, rows).T
    grid = grid[jax.random.permutation(jax.random.fold_in(own, 1), rows)]
    offset_by = jax.random.randint(jax.random.fold_in(own, 2), (rows, 1), 0, top)
    return jnp.take_along_axis(grid, (jnp.arange(top)[None, :] + offset_by) % top, axis=1)


def shares(count, total, most, slope, full):
    portions = [(1 << 20) // math.isqrt(grade ** slope) + 1 for grade in range(1, count + 1)]
    largest = most if full else min(most, max(-(-total // count), total * portions[0] // sum(portions)))
    least = 1 if total - largest >= count - 1 else 0
    holding, rest = [largest] + [least] * (count - 1), total - largest - least * (count - 1)
    while rest > 0:
        candidates = [i for i in range(1, count) if holding[i] < largest] or [i for i in range(1, count) if holding[i] < most]
        whole, budget = sum([portions[i] for i in candidates]), rest
        for i in candidates:
            extra = min(most - holding[i], max(1, budget * portions[i] // whole), rest)
            holding[i] = holding[i] + extra
            rest = rest - extra
    return np.array(holding)


def normal_values(key, extent, spread, most, pieces=(), held_as=jnp.bfloat16):
    loudness = shard_levels(key, extent, pieces, -0.22, 0.18) if pieces else 1.0
    result = jax.random.normal(key, extent, jnp.float32) * spread * loudness
    return jnp.minimum(jnp.maximum(result, -most), most).astype(held_as)


def setup_inputs(seed: int = 0) -> dict:
    seeds = jax.random.split(jax.random.key(seed), 7)
    grad_out = normal_values(seeds[0], (TOKENS, D), 1.0, 6.0, ((0, 8),))
    route_ids_keys = jax.random.split(jax.random.fold_in(seeds[1], 1), TOKENS // TOK_DEV)
    route_ids_turns = jax.random.permutation(jax.random.fold_in(seeds[1], 3), TOKENS // TOK_DEV)
    route_ids = jax.vmap(lambda own, number: assign_block(jax.random.fold_in(seeds[1], 2), own, number, TOK_DEV, EXPERTS, TOP, CAP, 2))(route_ids_keys, route_ids_turns).reshape((TOKENS, TOP))
    route_probs = jnp.clip(jnp.exp(math.log(0.5) - 3.224016 * jax.random.uniform(seeds[2], (TOKENS, TOP), jnp.float32) ** shard_levels(seeds[2], (TOKENS, TOP), ((0, 8),), -0.2, 0.2)), 0.019897461, 0.5).astype(jnp.bfloat16)
    gate_act = normal_values(seeds[3], (N_DP, EXPERTS, SLOTS, FF), 1.5, 8.0, ((0, 2), (1, 4), (3, 4)))
    up_act = normal_values(seeds[4], (N_DP, EXPERTS, SLOTS, FF), 1.0, 6.0, ((0, 2), (1, 4), (3, 4)))
    w_down = normal_values(seeds[5], (EXPERTS, FF, D), FF ** -0.5, 0.21875, ((0, 4), (1, 4)))
    return {"grad_out": grad_out, "route_ids": route_ids, "route_probs": route_probs, "gate_act": gate_act, "up_act": up_act, "w_down": w_down}


def expert_backward(inputs, grad_out):
    slot_token, slot_weight, gate_in, up_in, weight = inputs
    valid = slot_token >= 0
    picked = grad_out[jnp.maximum(slot_token, 0)]
    slot_rows = jnp.where(valid[:, :, None], picked, jnp.zeros_like(picked))
    grad_hidden = jnp.einsum("rsd,fd->rsf", slot_rows.astype(jnp.float32), weight.astype(jnp.float32))
    gate_pre = gate_in.astype(jnp.float32)
    up_pre = up_in.astype(jnp.float32)
    sigmoid_gate = jax.nn.sigmoid(gate_pre)
    silu_gate = gate_pre * sigmoid_gate
    hidden = (silu_gate * up_pre).astype(jnp.bfloat16)
    slot_dot = jnp.sum(grad_hidden * hidden.astype(jnp.float32), axis=2)
    grad_scaled = slot_weight[:, :, None] * grad_hidden
    grad_up = (grad_scaled * silu_gate).astype(jnp.bfloat16)
    grad_gate = (grad_scaled * up_pre * sigmoid_gate * (1.0 + gate_pre * (1.0 - sigmoid_gate))).astype(jnp.bfloat16)
    scaled_rows = (slot_weight[:, :, None] * slot_rows.astype(jnp.float32)).astype(jnp.bfloat16)
    replica_grad = jnp.einsum("rsf,rsd->rfd", hidden.astype(jnp.float32), scaled_rows.astype(jnp.float32))
    rounded = lax.optimization_barrier(replica_grad.astype(jnp.bfloat16))
    grad_weight = jnp.sum(rounded.astype(jnp.float32), axis=0).astype(jnp.bfloat16)
    return grad_gate, grad_up, grad_weight, slot_dot


def reference(grad_out, route_ids, route_probs, gate_act, up_act, w_down):
    block_count = N_EXPERT * N_DP
    route_count = TOK_DEV * TOP
    routes_block = route_ids.reshape(block_count, route_count).astype(jnp.int32)
    matches = (routes_block[:, :, None] == jnp.arange(EXPERTS, dtype=jnp.int32)[None, None, :]).astype(jnp.int32)
    earlier = jnp.cumsum(matches, axis=1) - matches
    position = jnp.sum(earlier * matches, axis=2).astype(jnp.int32)
    block_index = jnp.arange(block_count, dtype=jnp.int32)[:, None]
    source = block_index // N_DP
    replica = jnp.broadcast_to(block_index % N_DP, (block_count, route_count))
    slot = (source * CAP + position).astype(jnp.int32)
    token_index = (block_index * TOK_DEV + jnp.arange(route_count, dtype=jnp.int32)[None, :] // TOP).astype(jnp.int32)
    flat_replica = replica.reshape(-1)
    flat_expert = routes_block.reshape(-1)
    flat_slot = slot.reshape(-1)
    slot_token = jnp.full((N_DP, EXPERTS, SLOTS), -1, jnp.int32).at[flat_replica, flat_expert, flat_slot].set(token_index.reshape(-1))
    slot_weight = jnp.zeros((N_DP, EXPERTS, SLOTS), jnp.float32).at[flat_replica, flat_expert, flat_slot].set(route_probs.reshape(-1).astype(jnp.float32))
    inputs = (jnp.transpose(slot_token, (1, 0, 2)), jnp.transpose(slot_weight, (1, 0, 2)),
              jnp.transpose(gate_act, (1, 0, 2, 3)), jnp.transpose(up_act, (1, 0, 2, 3)), w_down)
    grad_gate, grad_up, grad_w_down, slot_dot = lax.map(lambda item: expert_backward(item, grad_out), inputs)
    grad_gate = jnp.transpose(grad_gate, (1, 0, 2, 3))
    grad_up = jnp.transpose(grad_up, (1, 0, 2, 3))
    slot_dot = jnp.transpose(slot_dot, (1, 0, 2))
    grad_probs = slot_dot[flat_replica, flat_expert, flat_slot].reshape(TOKENS, TOP)
    return (grad_gate, grad_up, grad_w_down, grad_probs)
```

```python
import functools
import jax
import jax.numpy as jnp
from jax import lax
from jax.experimental import pallas as pl
from jax.experimental.pallas import tpu as pltpu
from jax.sharding import PartitionSpec as P


def on_device_wide(grad_out, route_ids, route_probs, gate_act, up_act, w_down):
    tok_count = grad_out.shape[0]
    top_count = route_ids.shape[1]
    expert_count = lax.axis_size("expert")
    tensor_count = lax.axis_size("tensor")
    local_experts = w_down.shape[0]
    experts = local_experts * expert_count
    slot_count = gate_act.shape[2]
    capacity = slot_count // expert_count
    model_width = grad_out.shape[1]
    quarter = model_width // tensor_count
    route_flat = route_ids.reshape(-1)
    expert_iota = lax.broadcasted_iota(jnp.int32, (1, experts), 1)
    matches = (route_flat[:, None] == expert_iota).astype(jnp.int32)
    earlier = jnp.cumsum(matches, axis=0) - matches
    position = jnp.sum(earlier * matches, axis=1)
    target = route_flat * capacity + position
    cell_iota = lax.broadcasted_iota(jnp.int32, (1, experts * capacity), 1)
    chosen = target[:, None] == cell_iota
    chosen_weight = chosen.astype(jnp.float32)
    token_chosen = jnp.sum(
        chosen_weight.reshape(tok_count, top_count, experts * capacity), axis=1
    ).astype(jnp.bfloat16)
    own_columns = lax.dynamic_slice_in_dim(grad_out, lax.axis_index("tensor") * quarter, quarter, 1)
    send_rows = jnp.einsum(
        "nf,nd->fd", token_chosen, own_columns, preferred_element_type=jnp.float32
    ).astype(jnp.bfloat16)
    send_probs = jnp.sum(
        chosen_weight * route_probs.reshape(-1).astype(jnp.float32)[:, None], axis=0
    ).astype(jnp.bfloat16)
    send_rows = send_rows.reshape(expert_count, local_experts, capacity, quarter)
    send_probs = send_probs.reshape(expert_count, local_experts, capacity)
    arrived_rows, arrived_probs = (
        lax.all_to_all(send_rows, "expert", split_axis=0, concat_axis=0, tiled=True),
        lax.all_to_all(send_probs, "expert", split_axis=0, concat_axis=0, tiled=True),
    )
    gathered = lax.all_gather(arrived_rows, "tensor", axis=3, tiled=True)
    slot_rows = jnp.transpose(gathered, (1, 0, 2, 3)).reshape(
        local_experts, slot_count, model_width
    )
    slot_probs = (
        jnp.transpose(arrived_probs, (1, 0, 2))
        .reshape(local_experts, slot_count)
        .astype(jnp.float32)
    )
    gate_pre = gate_act[0].astype(jnp.float32)
    up_pre = up_act[0].astype(jnp.float32)
    grad_hidden = jnp.einsum("jsd,jfd->jsf", slot_rows, w_down, preferred_element_type=jnp.float32)
    sigmoid_gate = jax.nn.sigmoid(gate_pre)
    silu_gate = gate_pre * sigmoid_gate
    hidden = (silu_gate * up_pre).astype(jnp.bfloat16)
    partial_dot = jnp.sum(grad_hidden * hidden.astype(jnp.float32), axis=2)
    grad_scaled = slot_probs[:, :, None] * grad_hidden
    grad_up = (grad_scaled * silu_gate).astype(jnp.bfloat16)
    grad_gate = (
        grad_scaled * up_pre * sigmoid_gate * (1.0 + gate_pre * (1.0 - sigmoid_gate))
    ).astype(jnp.bfloat16)
    scaled_rows = (slot_probs[:, :, None] * slot_rows.astype(jnp.float32)).astype(jnp.bfloat16)
    replica_count = lax.axis_size("dp")
    column_count = model_width // replica_count
    split_rows = jnp.transpose(
        scaled_rows.reshape(local_experts, slot_count, replica_count, column_count), (2, 0, 1, 3)
    )
    columns = lax.all_to_all(split_rows, "dp", split_axis=0, concat_axis=0, tiled=True)
    initial = jnp.zeros((local_experts, hidden.shape[2], column_count), jnp.float32)
    hidden_block = lax.all_gather(hidden[None], "dp", axis=0, tiled=True)

    def add_member(member, summed):
        hid_one = lax.dynamic_index_in_dim(hidden_block, member, 0, keepdims=False)
        col_one = lax.dynamic_index_in_dim(columns, member, 0, keepdims=False)
        term = jnp.einsum("jsf,jsd->jfd", hid_one, col_one, preferred_element_type=jnp.float32)
        rounded = lax.optimization_barrier(term.astype(jnp.bfloat16))
        return summed + rounded.astype(jnp.float32)

    grad_weight = lax.fori_loop(0, hidden_block.shape[0], add_member, initial).astype(jnp.bfloat16)
    prob_cells = jnp.transpose(
        partial_dot.reshape(local_experts, expert_count, capacity), (1, 0, 2)
    )
    prob_cells = lax.psum(prob_cells, "tensor")
    returned = lax.all_to_all(prob_cells, "expert", split_axis=0, concat_axis=0, tiled=True)
    returned_flat = returned.reshape(-1)
    grad_probs = jnp.sum(jnp.where(chosen, returned_flat[None, :], 0.0), axis=1).reshape(
        tok_count, top_count
    )
    return (grad_gate[None], grad_up[None], grad_weight, grad_probs)


MESH = pl.DeviceIdType.MESH


def collect_kernel(sizes, x_ref, meta_ref, hid_ref, tok, oth, metas, hid_oth, local, zs, zr, ms, mr, hs, hr, xs, xr, ys, yr, vs, vr, cs, cr):
    tn, en, rn = sizes
    t, e, d = lax.axis_index("tensor"), lax.axis_index("expert"), lax.axis_index("dp")
    across = lax.rem(t + 2, tn)
    mate = t + 1 - 2 * lax.rem(t, 2)
    far = 1 - d
    barrier = pltpu.get_barrier_semaphore()
    others = []
    for i in range(en):
        for j in range(rn):
            if i or j:
                others.append((t, lax.rem(e + i, en), lax.rem(d + j, rn)))
    peers = others + [(across, e, d), (mate, e, d)]
    for peer in peers:
        pl.semaphore_signal(barrier, inc=1, device_id=peer, device_id_type=MESH)
    pl.semaphore_wait(barrier, len(peers))

    def send(src, dst, ssem, rsem, peer):
        copy = pltpu.make_async_remote_copy(
            src_ref=src, dst_ref=dst, send_sem=ssem, recv_sem=rsem, device_id=peer, device_id_type=MESH
        )
        copy.start()
        return copy

    mine = [
        pltpu.make_async_copy(x_ref, tok.at[t, e], local.at[0]),
        pltpu.make_async_copy(meta_ref, metas.at[e, d], local.at[1]),
    ]
    for copy in mine:
        copy.start()
    z = [
        send(x_ref, tok.at[t, e], zs.at[j - 1], zr.at[j - 1], (t, lax.rem(e + j, en), d))
        for j in range(1, en)
    ]
    m = [send(meta_ref, metas.at[e, d], ms.at[i], mr.at[i], peer) for i, peer in enumerate(others)]
    y = [send(x_ref, tok.at[t, e], ys.at[0], yr.at[0], (across, e, d))]
    x = [send(x_ref.at[far], oth.at[t, e], xs.at[0], xr.at[0], (t, e, far))]
    for j in range(1, en):
        z[j - 1].wait_recv()
        b = lax.rem(e - j + en, en)
        x.append(send(tok.at[t, b, far], oth.at[t, b], xs.at[j], xr.at[j], (t, e, far)))
        y.append(send(tok.at[t, b], tok.at[t, b], ys.at[j], yr.at[j], (across, e, d)))
    h = send(hid_ref, hid_oth, hs, hr, (t, e, far))
    v = []
    for j in range(en):
        x[j].wait_recv()
        b = lax.rem(e - j + en, en)
        v.append(send(oth.at[t, b], oth.at[t, b], vs.at[j], vr.at[j], (across, e, d)))
    for copy in mine:
        copy.wait()
    c = [
        send(tok.at[t], tok.at[t], cs.at[0], cr.at[0], (mate, e, d)),
        send(oth.at[t], oth.at[t], cs.at[1], cr.at[1], (mate, e, d)),
    ]
    for copy in y:
        copy.wait_recv()
    c.append(send(tok.at[across], tok.at[across], cs.at[2], cr.at[2], (mate, e, d)))
    for copy in v:
        copy.wait_recv()
    c.append(send(oth.at[across], oth.at[across], cs.at[3], cr.at[3], (mate, e, d)))
    for copy in m + c + [h]:
        copy.wait_recv()
    for copy in z + m + y + x + v + c + [h]:
        copy.wait_send()


def return_kernel(sizes, x_ref, out, local, ss, rs):
    tn, en = sizes
    t, e, d = lax.axis_index("tensor"), lax.axis_index("expert"), lax.axis_index("dp")
    barrier = pltpu.get_barrier_semaphore()
    peers = []
    for i in range(tn):
        for j in range(en):
            if i or j:
                peers.append((lax.rem(t + i, tn), lax.rem(e + j, en), d))
    for peer in peers:
        pl.semaphore_signal(barrier, inc=1, device_id=peer, device_id_type=MESH)
    pl.semaphore_wait(barrier, len(peers))
    mine = pltpu.make_async_copy(x_ref.at[e], out.at[t, e], local)
    mine.start()
    copies = []
    for i, peer in enumerate(peers):
        copy = pltpu.make_async_remote_copy(
            src_ref=x_ref.at[peer[1]], dst_ref=out.at[t, e], send_sem=ss.at[i], recv_sem=rs.at[i],
            device_id=peer, device_id_type=MESH,
        )
        copy.start()
        copies.append(copy)
    mine.wait()
    for copy in copies:
        copy.wait()


def expert_kernel(rows, scaled, hid_own, hid_far, gate, up, prob, w, grad_gate, grad_up, grad_w, dot):
    slots = rows.shape[1]
    turned = lax.dot_general(
        w[0], rows[0], (((1,), (1,)), ((), ())), preferred_element_type=jnp.float32
    )
    grad_hidden = turned.T
    g = gate[0, 0].astype(jnp.float32)
    u = up[0, 0].astype(jnp.float32)
    s = jax.nn.sigmoid(g)
    silu = g * s
    hidden = hid_own[0]
    dot[0] = jnp.sum(grad_hidden * hidden.astype(jnp.float32), axis=1, keepdims=True)
    weighted = prob[0] * grad_hidden
    grad_up[0, 0] = (weighted * silu).astype(jnp.bfloat16)
    grad_gate[0, 0] = (weighted * u * s * (1.0 + g * (1.0 - s))).astype(jnp.bfloat16)
    both = jnp.concatenate([hidden.astype(jnp.float32), hid_far[0].astype(jnp.float32)], axis=0)
    both = both.T.astype(jnp.bfloat16)
    grad_w[0] = jnp.dot(both, scaled[0], preferred_element_type=jnp.float32).astype(jnp.bfloat16)


def on_device(grad_out, route_ids, route_probs, gate_act, up_act, w_down):
    tokens, width = grad_out.shape
    top = route_ids.shape[1]
    tn, en, rn = lax.axis_size("tensor"), lax.axis_size("expert"), lax.axis_size("dp")
    t, e, d = lax.axis_index("tensor"), lax.axis_index("expert"), lax.axis_index("dp")
    local, units, slots = w_down.shape[0], w_down.shape[1], gate_act.shape[2]
    cap = slots // en
    strip = width // (tn * rn)
    half = width // rn
    f32, bf16 = jnp.float32, jnp.bfloat16
    sem = pltpu.SemaphoreType.DMA
    vmem = pl.BlockSpec(memory_space=pltpu.VMEM)
    g = gate_act[0].astype(f32)
    hidden = (g * jax.nn.sigmoid(g) * up_act[0].astype(f32)).astype(bf16)
    parts = jnp.transpose(grad_out.reshape(tokens, rn, tn, strip), (2, 1, 0, 3))
    mine = lax.dynamic_index_in_dim(parts, t, 0, keepdims=False)
    meta = jnp.concatenate([route_ids.T.astype(f32), route_probs.T.astype(f32)], axis=1)
    tok, oth, metas, hid_far = pl.pallas_call(
        functools.partial(collect_kernel, (tn, en, rn)),
        out_shape=(
            jax.ShapeDtypeStruct((tn, en, rn, tokens, strip), bf16),
            jax.ShapeDtypeStruct((tn, en, tokens, strip), bf16),
            jax.ShapeDtypeStruct((en, rn) + meta.shape, f32),
            jax.ShapeDtypeStruct(hidden.shape, bf16),
        ),
        in_specs=[vmem] * 3,
        out_specs=(vmem,) * 4,
        scratch_shapes=[
            sem((2,)), sem((en - 1,)), sem((en - 1,)), sem((en * rn - 1,)), sem((en * rn - 1,)), sem, sem,
            sem((en,)), sem((en,)), sem((en,)), sem((en,)), sem((en,)), sem((en,)), sem((4,)), sem((4,)),
        ],
        compiler_params=pltpu.CompilerParams(collective_id=0, has_side_effects=True),
    )(mine, meta, hidden)

    ids = metas[..., :tokens].astype(jnp.int32)
    probs = metas[..., tokens:]
    here = e * local + jnp.arange(local, dtype=jnp.int32)
    hit = ids[:, :, :, None, :] == here[:, None]
    named = jnp.any(hit, axis=2)
    weight = jnp.sum(jnp.where(hit, probs[:, :, :, None, :], 0.0), axis=2)
    below = jnp.arange(tokens)[:, None] < jnp.arange(tokens)[None, :]
    position = jnp.einsum("erxn,nm->erxm", named.astype(bf16), below.astype(bf16), preferred_element_type=f32)
    place = jnp.where(named, position, -1.0)
    spots = place[:, :, :, None, :] == jnp.arange(cap, dtype=f32)[:, None]
    spots = jnp.transpose(spots, (1, 2, 0, 3, 4))
    carried = jnp.transpose(weight, (1, 2, 0, 3))[:, :, :, None, :]
    same = (jnp.arange(en)[:, None] == jnp.arange(en)[None, :])[None, None, :, None, :, None]
    one = (spots[:, :, :, :, None, :] & same).reshape(rn, local * slots, en * tokens)
    wide = jnp.where(spots, carried, 0.0)
    slot_probs = lax.dynamic_index_in_dim(jnp.sum(wide, axis=-1), d, 0, keepdims=False).reshape(local, slots, 1)
    wide = jnp.where(same, wide[:, :, :, :, None, :], 0.0).astype(bf16).reshape(rn, local * slots, en * tokens)
    pick = lambda a, i: lax.dynamic_index_in_dim(a, i, 0, keepdims=False)
    flat = jnp.transpose(tok, (1, 3, 2, 0, 4)).reshape(en * tokens, width)
    far_flat = jnp.transpose(oth, (1, 2, 0, 3)).reshape(en * tokens, half)
    near_flat = lax.dynamic_slice_in_dim(flat, d * half, half, 1)
    rows = jnp.dot(pick(one, d).astype(bf16), flat, preferred_element_type=f32).astype(bf16).reshape(local, slots, width)
    near = jnp.dot(pick(wide, d), near_flat, preferred_element_type=f32).astype(bf16).reshape(local, slots, half)
    far = jnp.dot(pick(wide, 1 - d), far_flat, preferred_element_type=f32).astype(bf16).reshape(local, slots, half)
    scaled = jnp.concatenate([near, far], axis=1)

    def block(*shape):
        return pl.BlockSpec((1,) + shape, lambda i: (i,) + (0,) * len(shape))

    act = pl.BlockSpec((1, 1, slots, units), lambda i: (0, i, 0, 0))
    act_shape = jax.ShapeDtypeStruct((1, local, slots, units), bf16)
    grad_gate, grad_up, grad_w, dot = pl.pallas_call(
        expert_kernel,
        grid=(local,),
        in_specs=[
            block(slots, width), block(2 * slots, half), block(slots, units), block(slots, units), act, act,
            block(slots, 1), block(units, width),
        ],
        out_specs=(act, act, block(units, half), block(slots, 1)),
        out_shape=(
            act_shape, act_shape,
            jax.ShapeDtypeStruct((local, units, half), bf16),
            jax.ShapeDtypeStruct((local, slots, 1), f32),
        ),
    )(rows, scaled, hidden, hid_far, gate_act, up_act, slot_probs, w_down)

    cells = jnp.transpose(dot.reshape(local, en, cap), (1, 0, 2)).reshape(en, local * cap)
    room = -(-local * cap // 1024) * 1024
    cells = jnp.pad(cells, ((0, 0), (0, room - local * cap))).reshape(en, room // 128, 128)
    back = pl.pallas_call(
        functools.partial(return_kernel, (tn, en)),
        out_shape=jax.ShapeDtypeStruct((tn,) + cells.shape, f32),
        in_specs=[vmem],
        out_specs=vmem,
        scratch_shapes=[sem, sem((tn * en - 1,)), sem((tn * en - 1,))],
        compiler_params=pltpu.CompilerParams(collective_id=1, has_side_effects=True),
    )(cells)
    back = jnp.sum(back, axis=0).reshape(en, room)[:, : local * cap].reshape(1, 1, -1)
    every = jnp.arange(en * local, dtype=jnp.int32)
    match = route_ids[:, :, None] == every
    count = jnp.any(match, axis=1)
    before = jnp.einsum("nx,nm->mx", count.astype(bf16), below.astype(bf16), preferred_element_type=f32)
    at = jnp.sum(jnp.where(match, before[:, None, :], 0.0), axis=2).astype(jnp.int32)
    target = route_ids * cap + at
    chosen = target[:, :, None] == jnp.arange(en * local * cap, dtype=jnp.int32)
    grad_probs = jnp.sum(jnp.where(chosen, back, 0.0), axis=2)
    return grad_gate, grad_up, grad_w, grad_probs


def solution(mesh):
    sizes = mesh.shape
    small = sizes["tensor"] == 4 and sizes["dp"] == 2 and sizes["expert"] <= 8
    placed = (
        P(("expert", "dp"), None),
        P(("expert", "dp"), None),
        P(("expert", "dp"), None),
        P("dp", "expert", None, "tensor"),
        P("dp", "expert", None, "tensor"),
        P("expert", "tensor", None),
    )
    return jax.shard_map(
        on_device if small else on_device_wide,
        mesh=mesh,
        in_specs=placed,
        out_specs=(
            P("dp", "expert", None, "tensor"),
            P("dp", "expert", None, "tensor"),
            P("expert", "tensor", "dp"),
            P(("expert", "dp"), None),
        ),
        check_vma=False,
    )
```
